32 devices in a mesh: gx: 2 (over core), gy: 4 (over y, x), gz: 4 (over z).
Axes of the slice: x: 2, y: 2, z: 4, core: 2. Of those that a mesh axis runs over, the one named last changes fastest.
Arguments:
- queries: bfloat16 [128, 32, 128], P(None, 'gy'), may hold values from -6 to 6
- passages: bfloat16 [1024, 256, 128], P('gx', 'gz'), may hold values from -0.5 to 0.5
- passage_len: int32 [1024], P('gx'), may hold values from 32 to 256
- query_len: int32 [128], replicated, may hold values from 8 to 32
Outputs:
- log_probs: float32 [128, 1024], P(None, ('gx', 'gz'))
The draws below stay inside these ranges and needn't reach their ends.
All inputs are finite; a program needn't handle non-finite values.
Results may differ from the reference program's by a relative error of at most 0.0003.
Values sent between devices are 32-bit elements; how exact they have to be, the bound alone decides.
A program may use at most 64 MiB of HBM per device.

```python
import math
import jax
import jax.numpy as jnp
from jax import lax

DIM = 128
NQ = 128
LQ = 32
LP = 256
NP = 1024


def draw_queries(key, part):
    noise_key = jax.random.fold_in(key, 11)
    values = jnp.clip(jax.random.normal(noise_key, (NQ, LQ, DIM), jnp.float32), -6.0, 6.0)
    return values.astype(jnp.bfloat16)


def draw_passages(key, part):
    noise_key = jax.random.fold_in(key, 21)
    values = jax.random.normal(noise_key, (NP, LP, DIM), jnp.float32) * DIM ** (-0.5)
    values = jnp.clip(values, -0.5, 0.5)
    return values.astype(jnp.bfloat16)


def set_ends(entries, stream_key, smallest, high):
    spot = [jax.random.randint(jax.random.fold_in(stream_key, axis), (), 0, length) for axis, length in enumerate(entries.shape)]
    main_axis = entries.shape.index(max(entries.shape))
    beside = spot[:main_axis] + [(spot[main_axis] + 1) % entries.shape[main_axis]] + spot[main_axis + 1:]
    return entries.at[tuple(spot)].set(smallest).at[tuple(beside)].set(high)


def setup_inputs(seed: int = 0) -> dict:
    arg_keys = jax.random.split(jax.random.key(seed), 5)
    queries = draw_queries(jax.random.fold_in(arg_keys[4], 71), 0)
    passages = draw_passages(jax.random.fold_in(arg_keys[4], 71), 0)
    passage_len = set_ends(jax.random.randint(arg_keys[2], (NP,), LP // 8, LP + 1), jax.random.fold_in(arg_keys[2], 1), LP // 8, LP).astype(jnp.int32)
    query_len = set_ends(jax.random.randint(arg_keys[3], (NQ,), max(1, LQ // 4), LQ + 1), jax.random.fold_in(arg_keys[3], 1), max(1, LQ // 4), LQ).astype(jnp.int32)
    return dict(queries=queries, passages=passages, passage_len=passage_len, query_len=query_len)


masked_low = -1.0e30


def reference(queries, passages, passage_len, query_len):
    flat_queries = queries.reshape(NQ * LQ, DIM)
    per_block = math.gcd(NP, 32)
    num_blocks = NP // per_block
    tile_stack = passages.reshape(num_blocks, per_block * LP, DIM)
    length_stack = passage_len.reshape(num_blocks, per_block)
    query_used = jnp.arange(LQ, dtype=jnp.int32)[None, :] < query_len[:, None]
    token_ids = jnp.arange(LP, dtype=jnp.int32)

    def block_scores(packed):
        passage_tile, tile_len = packed
        scores = jnp.dot(flat_queries, passage_tile.T, preferred_element_type=jnp.float32)
        scores = scores.reshape(NQ * LQ, per_block, LP)
        usable = token_ids[None, :] < tile_len[:, None]
        scores = jnp.where(usable[None], scores, masked_low)
        maxima = jnp.max(scores, axis=2).reshape(NQ, LQ, per_block)
        return jnp.sum(jnp.where(query_used[:, :, None], maxima, 0.0), axis=1)

    pieces = lax.map(block_scores, (tile_stack, length_stack))
    maxsim = jnp.transpose(pieces, (1, 0, 2)).reshape(NQ, NP)
    highest = jnp.max(maxsim, axis=1, keepdims=True)
    summed = jnp.sum(jnp.exp(maxsim - highest), axis=1, keepdims=True)
    return maxsim - (highest + jnp.log(summed))
```

```python
import functools

import jax
import jax.numpy as jnp
from jax import lax
from jax.experimental import pallas as pl
from jax.experimental.pallas import tpu as pltpu
from jax.sharding import PartitionSpec as P

masked_low = -1e30
MESH = pl.DeviceIdType.MESH
HOP_LAG = 3
PEER_LAG = 3
PER_CHUNK = 16


def kernel(
    sizes,
    queries,
    lengths,
    query_len,
    passages,
    out,
    x,
    masked_x,
    wide_queries,
    query_columns,
    limits,
    own_low,
    own_high,
    got_low,
    got_high,
    partials,
    forward,
    total,
    stats,
    load_sem,
    z_send,
    low_recv,
    high_recv,
    peer_send,
    peer_recv,
    forward_send,
    forward_recv,
    stat_send,
    stat_recv,
):
    nx, ny, nz = sizes
    gx, gy, gz = (lax.axis_index(name) for name in ("gx", "gy", "gz"))
    passage_count, token_count, width = x.shape
    query_count, query_rows, _ = queries.shape
    chunks, per_chunk, row_count = own_low.shape
    half_blocks = nz // 2
    per_block = chunks // half_blocks
    block_rows = passage_count // nz
    group = nx * nz
    me = gx * nz + gz

    def low_start(c):
        return (half_blocks - 1 - c // per_block) * block_rows + (c % per_block) * per_chunk

    def high_start(c):
        return half_blocks * block_rows + c * per_chunk

    def member(turn):
        index = lax.rem(me + turn, group)
        return index, (index // nz, gy, lax.rem(index, nz))

    barrier = pltpu.get_barrier_semaphore()
    for turn in range(1, ny):
        pl.semaphore_signal(
            barrier, inc=1, device_id={"gy": lax.rem(gy + turn, ny)}, device_id_type=MESH
        )

    def greet(turn, carry):
        pl.semaphore_signal(barrier, inc=1, device_id=member(turn)[1], device_id_type=MESH)
        return carry

    lax.fori_loop(1, group, greet, 0)

    def load(start, index):
        rows = pl.ds(start, per_chunk)
        return pltpu.make_async_copy(passages.at[rows], x.at[rows], load_sem.at[index])

    def start_loads(c, carry):
        load(low_start(c), c).start()
        load(high_start(c), chunks + c).start()
        return carry

    lax.fori_loop(0, chunks, start_loads, 0)

    wide_queries[...] = queries[...].astype(jnp.float32).reshape(row_count, width)
    for i in range(query_rows):
        tile = wide_queries[pl.ds(i, query_count, stride=query_rows), :]
        query_columns[:, i * query_count : (i + 1) * query_count] = tile.T.astype(jnp.bfloat16)

    first_token = (gz * token_count).astype(jnp.float32)
    for b in range(passage_count // 128):
        row = lengths[b : b + 1, :].astype(jnp.float32) - first_token
        limits[b * 128 : (b + 1) * 128, :] = jnp.broadcast_to(row, (128, 128)).T

    pl.semaphore_wait(barrier, ny - 1 + group - 1)

    token_ids = lax.broadcasted_iota(jnp.int32, (token_count, width), 0).astype(jnp.float32)
    tile_columns = 256

    def compute(own, c, start, index):
        load(start, index).wait()
        for p in range(per_chunk):
            tokens = x[start + p].astype(jnp.float32)
            usable = token_ids < limits[pl.ds(start + p, 1), :]
            tokens = jnp.where(usable, tokens, tokens[0:1, :])
            masked_x[p * token_count : (p + 1) * token_count, :] = tokens.astype(jnp.bfloat16)
        limit = limits[pl.ds(start, per_chunk), :]
        any_used = jnp.concatenate([limit] * (tile_columns // 128), axis=1) > 0.0
        for t in range(row_count // tile_columns):
            columns = slice(t * tile_columns, (t + 1) * tile_columns)
            scores = jnp.dot(
                masked_x[...], query_columns[:, columns], preferred_element_type=jnp.float32
            )
            best = jnp.max(scores.reshape(per_chunk, token_count, tile_columns), axis=1)
            own[c, :, columns] = jnp.where(any_used, best, masked_low)

    def z_copy(own, got, recv, send_index, c, target):
        return pltpu.make_async_remote_copy(
            src_ref=own.at[c],
            dst_ref=got.at[c],
            send_sem=z_send.at[send_index],
            recv_sem=recv.at[c],
            device_id={"gz": target},
            device_id_type=MESH,
        )

    def peer_copy(turn, slot, block, where):
        return pltpu.make_async_remote_copy(
            src_ref=partials.at[slot, where],
            dst_ref=partials.at[slot, where],
            send_sem=peer_send.at[turn],
            recv_sem=peer_recv.at[slot, block],
            device_id={"gy": lax.rem(gy + turn, ny)},
            device_id_type=MESH,
        )

    def finalise(own, c):
        counted = query_len[...] - gy * query_rows
        so_far = jnp.zeros((per_chunk, query_count), jnp.float32)
        for i in range(query_rows):
            values = own[c, :, i * query_count : (i + 1) * query_count]
            so_far = so_far + jnp.where(counted > i, values, 0.0)
        partials[gy, c] = so_far
        for turn in range(1, ny):
            peer_copy(turn, gy, c // per_block, c).start()

    def block_total(block):
        where = pl.ds(block * per_block, per_block)
        for turn in range(1, ny):
            slot = lax.rem(gy + turn, ny)
            peer_copy(turn, slot, block, where).wait_recv()
        summed = partials[0, where]
        for slot in range(1, ny):
            summed = summed + partials[slot, where]
        return summed.reshape(block_rows, query_count)

    def forward_copy(block):
        target = jnp.where(gz == 0, half_blocks - 1 - block, half_blocks + block)
        return pltpu.make_async_remote_copy(
            src_ref=forward.at[block],
            dst_ref=total,
            send_sem=forward_send.at[block],
            recv_sem=forward_recv,
            device_id={"gz": target},
            device_id_type=MESH,
        )

    at_end = (gz == 0) | (gz == nz - 1)

    def step(s, carry):
        @pl.when(s < chunks)
        def _():
            compute(own_low, s, low_start(s), s)
            compute(own_high, s, high_start(s), chunks + s)

        def travel(own, got, recv, send_index, c, is_first, is_last, target):
            @pl.when((c >= 0) & (c < chunks))
            def _():
                @pl.when(jnp.logical_not(is_first))
                def _():
                    z_copy(own, got, recv, send_index, c, target).wait_recv()
                    own[c] = jnp.maximum(own[c], got[c])

                @pl.when(jnp.logical_not(is_last))
                def _():
                    z_copy(own, got, recv, send_index, c, target).start()

                @pl.when(is_last)
                def _():
                    finalise(own, c)

        first, last = gz == 0, gz == nz - 1
        down = lax.rem(gz + nz - 1, nz)
        up = lax.rem(gz + 1, nz)
        travel(own_low, got_low, low_recv, 0, s - HOP_LAG * (nz - 1 - gz), last, first, down)
        travel(own_high, got_high, high_recv, 1, s - HOP_LAG * gz, first, last, up)

        ready = s - HOP_LAG * (nz - 1) - PEER_LAG
        for block in range(half_blocks - 1):
            @pl.when(at_end & (ready == (block + 1) * per_block - 1))
            def _():
                forward[block] = block_total(block)
                forward_copy(block).start()

        return carry

    lax.fori_loop(0, chunks + HOP_LAG * (nz - 1), step, 0)

    @pl.when(at_end)
    def _():
        total[...] = block_total(half_blocks - 1)

    @pl.when(jnp.logical_not(at_end))
    def _():
        forward_copy(0).wait_recv()

    scores = total[...]
    top = jnp.max(scores, axis=0, keepdims=True)
    summed = jnp.sum(jnp.exp(scores - top), axis=0, keepdims=True)
    row_ids = lax.broadcasted_iota(jnp.int32, stats.shape[1:], 0)
    stats[me] = jnp.where(row_ids == 0, top, summed)

    def stat_copy(slot, turn):
        return pltpu.make_async_remote_copy(
            src_ref=stats.at[slot],
            dst_ref=stats.at[slot],
            send_sem=stat_send.at[turn],
            recv_sem=stat_recv.at[slot],
            device_id=member(turn)[1],
            device_id_type=MESH,
        )

    def send_stats(turn, carry):
        stat_copy(me, turn).start()
        return carry

    lax.fori_loop(1, group, send_stats, 0)

    def wait_stats(turn, carry):
        stat_copy(member(turn)[0], turn).wait_recv()
        return carry

    lax.fori_loop(1, group, wait_stats, 0)
    tops = stats[:, 0, :]
    highest = jnp.max(tops, axis=0, keepdims=True)
    everything = jnp.sum(stats[:, 1, :] * jnp.exp(tops - highest), axis=0, keepdims=True)
    out[...] = (scores - (highest + jnp.log(everything))).T

    @pl.when(gz > 0)
    def _():
        whole = pl.ds(0, chunks)
        z_copy(own_low, got_low, low_recv, 0, whole, 0).wait_send()

    @pl.when(gz < nz - 1)
    def _():
        whole = pl.ds(0, chunks)
        z_copy(own_high, got_high, high_recv, 1, whole, 0).wait_send()

    @pl.when(at_end)
    def _():
        for turn in range(1, ny):
            peer_copy(turn, gy, 0, pl.ds(0, chunks)).wait_send()
        for block in range(half_blocks - 1):
            forward_copy(block).wait_send()

    def drain_stats(turn, carry):
        stat_copy(me, turn).wait_send()
        return carry

    lax.fori_loop(1, group, drain_stats, 0)


def shards(sizes, queries, passages, passage_len, query_len):
    nx, ny, nz = sizes
    query_count, query_rows, width = queries.shape
    passage_count, token_count, _ = passages.shape
    row_count = query_count * query_rows
    block_rows = passage_count // nz
    per_chunk = PER_CHUNK
    chunks = passage_count // 2 // per_chunk
    half_blocks = nz // 2
    maxima = pltpu.VMEM((chunks, per_chunk, row_count), jnp.float32)
    dma = pltpu.SemaphoreType.DMA
    vmem = pl.BlockSpec(memory_space=pltpu.VMEM)
    return pl.pallas_call(
        functools.partial(kernel, sizes),
        out_shape=jax.ShapeDtypeStruct((query_count, block_rows), jnp.float32),
        in_specs=[vmem, vmem, vmem, pl.BlockSpec(memory_space=pl.ANY)],
        out_specs=vmem,
        scratch_shapes=[
            pltpu.VMEM(passages.shape, passages.dtype),
            pltpu.VMEM((per_chunk * token_count, width), jnp.bfloat16),
            pltpu.VMEM((row_count, width), jnp.float32),
            pltpu.VMEM((width, row_count), jnp.bfloat16),
            pltpu.VMEM((passage_count, 128), jnp.float32),
            maxima,
            maxima,
            maxima,
            maxima,
            pltpu.VMEM((ny, chunks, per_chunk, query_count), jnp.float32),
            pltpu.VMEM((max(1, half_blocks - 1), block_rows, query_count), jnp.float32),
            pltpu.VMEM((block_rows, query_count), jnp.float32),
            pltpu.VMEM((nx * nz, 8, query_count), jnp.float32),
            dma((2 * chunks,)),
            dma((2,)),
            dma((chunks,)),
            dma((chunks,)),
            dma((ny,)),
            dma((ny, half_blocks)),
            dma((max(1, half_blocks - 1),)),
            dma,
            dma((nx * nz,)),
            dma((nx * nz,)),
        ],
        compiler_params=pltpu.CompilerParams(
            collective_id=0, has_side_effects=True, vmem_limit_bytes=48 * 1024 * 1024
        ),
    )(
        queries,
        passage_len.reshape(passage_count // 128, 128),
        query_len.reshape(1, query_count),
        passages,
    )


def solution(mesh):
    sizes = tuple(mesh.shape[name] for name in ("gx", "gy", "gz"))
    return jax.shard_map(
        functools.partial(shards, sizes),
        mesh=mesh,
        in_specs=(P(None, "gy", None), P("gx", "gz", None), P("gx"), P()),
        out_specs=P(None, ("gx", "gz")),
        check_vma=False,
    )
```

```python
import functools

import jax
import jax.numpy as jnp
from jax import lax
from jax.experimental import pallas as pl
from jax.experimental.pallas import tpu as pltpu
from jax.sharding import PartitionSpec as P

masked_low = -1e30
MESH = pl.DeviceIdType.MESH
HOP_LAG = 4
PEER_LAG = 3
PER_CHUNK = 16
PARTS = 2


def kernel(
    sizes,
    queries_in,
    lengths_in,
    query_len_in,
    passages,
    out,
    queries,
    lengths,
    query_len,
    x,
    masked_x,
    wide_queries,
    query_columns,
    limits,
    own_low,
    own_high,
    got_low,
    got_high,
    partials,
    forward,
    total,
    stats,
    small_sem,
    load_sem,
    z_send,
    low_recv,
    high_recv,
    peer_send,
    peer_recv,
    forward_send,
    forward_recv,
    stat_send,
    stat_recv,
):
    nx, ny, nz = sizes
    gx, gy, gz = (lax.axis_index(name) for name in ("gx", "gy", "gz"))
    passage_count, token_count, width = x.shape
    query_count, query_rows, _ = queries.shape
    slots, per_chunk, row_count = own_low.shape
    chunks = slots - 1
    part_rows = per_chunk // PARTS
    half_blocks = nz // 2
    per_block = chunks // half_blocks
    block_rows = passage_count // nz
    group = nx * nz
    me = gx * nz + gz

    def low_start(c):
        return (half_blocks - 1 - c // per_block) * block_rows + (c % per_block) * per_chunk

    def high_start(c):
        return half_blocks * block_rows + c * per_chunk

    def member(turn):
        index = lax.rem(me + turn, group)
        return index, (index // nz, gy, lax.rem(index, nz))

    barrier = pltpu.get_barrier_semaphore()
    for turn in range(1, ny):
        pl.semaphore_signal(
            barrier, inc=1, device_id={"gy": lax.rem(gy + turn, ny)}, device_id_type=MESH
        )

    def greet(turn, carry):
        pl.semaphore_signal(barrier, inc=1, device_id=member(turn)[1], device_id_type=MESH)
        return carry

    lax.fori_loop(1, group, greet, 0)

    small = [
        pltpu.make_async_copy(source, target, small_sem.at[index])
        for index, (source, target) in enumerate(
            ((queries_in, queries), (lengths_in, lengths), (query_len_in, query_len))
        )
    ]
    for copy in small:
        copy.start()

    def load(start, index):
        rows = pl.ds(start, per_chunk)
        return pltpu.make_async_copy(passages.at[rows], x.at[rows], load_sem.at[index])

    def start_loads(c, carry):
        load(low_start(c), c).start()
        load(high_start(c), chunks + c).start()
        return carry

    lax.fori_loop(0, chunks, start_loads, 0)

    for copy in small:
        copy.wait()

    wide_queries[...] = queries[...].astype(jnp.float32).reshape(row_count, width)
    for i in range(query_rows):
        tile = wide_queries[pl.ds(i, query_count, stride=query_rows), :]
        query_columns[:, i * query_count : (i + 1) * query_count] = tile.T.astype(jnp.bfloat16)

    first_token = (gz * token_count).astype(jnp.float32)
    for b in range(passage_count // 128):
        row = lengths[b : b + 1, :].astype(jnp.float32) - first_token
        limits[b * 128 : (b + 1) * 128, :] = jnp.broadcast_to(row, (128, 128)).T

    token_ids = lax.broadcasted_iota(jnp.int32, (token_count, width), 0).astype(jnp.float32)
    tile_columns = 256

    def compute(c):
        starts = (low_start(c), high_start(c))
        limit = []
        for half, start in enumerate(starts):
            for p in range(per_chunk):
                tokens = x[start + p].astype(jnp.float32)
                usable = token_ids < limits[pl.ds(start + p, 1), :]
                tokens = jnp.where(usable, tokens, tokens[0:1, :])
                row = (half * per_chunk + p) * token_count
                masked_x[row : row + token_count, :] = tokens.astype(jnp.bfloat16)
            limit.append(limits[pl.ds(start, per_chunk), :])
        limit = jnp.concatenate(limit, axis=0)
        any_used = jnp.concatenate([limit] * (tile_columns // 128), axis=1) > 0.0
        for t in range(row_count // tile_columns):
            columns = slice(t * tile_columns, (t + 1) * tile_columns)
            scores = jnp.dot(
                masked_x[...], query_columns[:, columns], preferred_element_type=jnp.float32
            )
            best = jnp.max(scores.reshape(2 * per_chunk, token_count, tile_columns), axis=1)
            best = jnp.where(any_used, best, masked_low)
            own_low[c, :, columns] = best[:per_chunk]
            own_high[c, :, columns] = best[per_chunk:]

    class Flow:
        def __init__(self, own, got, recv, send_index, hops, is_last, target):
            self.own, self.got, self.recv, self.send_index = own, got, recv, send_index
            self.is_first, self.is_last, self.target = hops == 0, is_last, target
            self.lag = HOP_LAG * hops

        def copy(self, source, c, part):
            rows = pl.ds(part * part_rows, part_rows)
            return pltpu.make_async_remote_copy(
                src_ref=source.at[c, rows],
                dst_ref=self.got.at[c, rows],
                send_sem=z_send.at[self.send_index],
                recv_sem=self.recv.at[c, part],
                device_id={"gz": self.target},
                device_id_type=MESH,
            )

        def merge(self, c, rows):
            self.got[c, rows] = jnp.maximum(self.got[c, rows], self.own[c, rows])

        def pass_on(self, c, part):
            @pl.when(jnp.logical_not(self.is_last))
            def _():
                self.copy(self.got, c, part).start()

            @pl.when(self.is_last)
            def _():
                finalise(self.got, c, part)

    first, last = gz == 0, gz == nz - 1
    low = Flow(own_low, got_low, low_recv, 0, nz - 1 - gz, first, lax.rem(gz + nz - 1, nz))
    high = Flow(own_high, got_high, high_recv, 1, gz, last, lax.rem(gz + 1, nz))
    flows = (low, high)

    def peer_copy(turn, slot, block, where):
        return pltpu.make_async_remote_copy(
            src_ref=partials.at[(slot, *where)],
            dst_ref=partials.at[(slot, *where)],
            send_sem=peer_send.at[turn],
            recv_sem=peer_recv.at[slot, block],
            device_id={"gy": lax.rem(gy + turn, ny)},
            device_id_type=MESH,
        )

    def finalise(merged, c, part):
        rows = pl.ds(part * part_rows, part_rows)
        counted = query_len[...] - gy * query_rows
        so_far = jnp.zeros((part_rows, query_count), jnp.float32)
        for i in range(query_rows):
            values = merged[c, rows, i * query_count : (i + 1) * query_count]
            so_far = so_far + jnp.where(counted > i, values, 0.0)
        partials[gy, c, rows] = so_far
        for turn in range(1, ny):
            peer_copy(turn, gy, c // per_block, (c, rows)).start()

    def block_total(block):
        where = pl.ds(block * per_block, per_block)
        for turn in range(1, ny):
            slot = lax.rem(gy + turn, ny)
            peer_copy(turn, slot, block, (where,)).wait_recv()
        summed = partials[0, where]
        for slot in range(1, ny):
            summed = summed + partials[slot, where]
        return summed.reshape(block_rows, query_count)

    def forward_copy(block):
        target = jnp.where(gz == 0, half_blocks - 1 - block, half_blocks + block)
        return pltpu.make_async_remote_copy(
            src_ref=forward.at[block],
            dst_ref=total,
            send_sem=forward_send.at[block],
            recv_sem=forward_recv,
            device_id={"gz": target},
            device_id_type=MESH,
        )

    at_end = (gz == 0) | (gz == nz - 1)

    def forward_ready_block(s):
        ready = s - HOP_LAG * (nz - 1) - PEER_LAG
        for block in range(half_blocks - 1):
            @pl.when(at_end & (ready == (block + 1) * per_block - 1))
            def _():
                forward[block] = block_total(block)
                forward_copy(block).start()

    def step(s, carry):
        load(low_start(s), s).wait()
        load(high_start(s), chunks + s).wait()
        waiting = []
        for flow in flows:
            c = s - flow.lag
            merging = jnp.logical_not(flow.is_first) & (c >= 0)
            waiting.append((flow, c, merging))

            @pl.when(merging)
            def _():
                for part in range(PARTS):
                    flow.copy(flow.got, c, part).wait_recv()

        for flow, c, merging in waiting:
            flow.merge(jnp.where(merging, c, chunks), pl.ds(0, per_chunk))
        compute(s)

        @pl.when(s == 0)
        def _():
            pl.semaphore_wait(barrier, ny - 1 + group - 1)

        for flow, c, merging in waiting:
            @pl.when(merging)
            def _():
                for part in range(PARTS):
                    flow.pass_on(c, part)

            @pl.when(flow.is_first)
            def _():
                for part in range(PARTS):
                    flow.copy(flow.own, s, part).start()

        forward_ready_block(s)
        return carry

    lax.fori_loop(0, chunks, step, 0)

    def drain(s, carry):
        for flow in flows:
            c = s - flow.lag

            @pl.when(jnp.logical_not(flow.is_first) & (c >= 0) & (c < chunks))
            def _():
                for part in range(PARTS):
                    flow.copy(flow.got, c, part).wait_recv()
                    flow.merge(c, pl.ds(part * part_rows, part_rows))
                    flow.pass_on(c, part)

        forward_ready_block(s)
        return carry

    lax.fori_loop(chunks, chunks + HOP_LAG * (nz - 1), drain, 0)

    @pl.when(at_end)
    def _():
        total[...] = block_total(half_blocks - 1)

    @pl.when(jnp.logical_not(at_end))
    def _():
        forward_copy(0).wait_recv()

    scores = total[...]
    top = jnp.max(scores, axis=0, keepdims=True)
    summed = jnp.sum(jnp.exp(scores - top), axis=0, keepdims=True)
    row_ids = lax.broadcasted_iota(jnp.int32, stats.shape[1:], 0)
    stats[me] = jnp.where(row_ids == 0, top, summed)

    def stat_copy(slot, turn):
        return pltpu.make_async_remote_copy(
            src_ref=stats.at[slot],
            dst_ref=stats.at[slot],
            send_sem=stat_send.at[turn],
            recv_sem=stat_recv.at[slot],
            device_id=member(turn)[1],
            device_id_type=MESH,
        )

    def send_stats(turn, carry):
        stat_copy(me, turn).start()
        return carry

    lax.fori_loop(1, group, send_stats, 0)

    def wait_stats(turn, carry):
        stat_copy(member(turn)[0], turn).wait_recv()
        return carry

    lax.fori_loop(1, group, wait_stats, 0)
    tops = stats[:, 0, :]
    highest = jnp.max(tops, axis=0, keepdims=True)
    everything = jnp.sum(stats[:, 1, :] * jnp.exp(tops - highest), axis=0, keepdims=True)
    out[...] = (scores - (highest + jnp.log(everything))).T

    for flow in flows:
        @pl.when(jnp.logical_not(flow.is_last))
        def _():
            whole = pl.ds(0, chunks)
            pltpu.make_async_remote_copy(
                src_ref=flow.got.at[whole],
                dst_ref=flow.got.at[whole],
                send_sem=z_send.at[flow.send_index],
                recv_sem=flow.recv.at[0, 0],
                device_id={"gz": flow.target},
                device_id_type=MESH,
            ).wait_send()

    @pl.when(at_end)
    def _():
        for turn in range(1, ny):
            peer_copy(turn, gy, 0, (pl.ds(0, chunks),)).wait_send()
        for block in range(half_blocks - 1):
            forward_copy(block).wait_send()

    def drain_stats(turn, carry):
        stat_copy(me, turn).wait_send()
        return carry

    lax.fori_loop(1, group, drain_stats, 0)


def shards(sizes, queries, passages, passage_len, query_len):
    nx, ny, nz = sizes
    query_count, query_rows, width = queries.shape
    passage_count, token_count, _ = passages.shape
    row_count = query_count * query_rows
    block_rows = passage_count // nz
    per_chunk = PER_CHUNK
    chunks = passage_count // 2 // per_chunk
    half_blocks = nz // 2
    maxima = pltpu.VMEM((chunks + 1, per_chunk, row_count), jnp.float32)
    dma = pltpu.SemaphoreType.DMA
    anywhere = pl.BlockSpec(memory_space=pltpu.HBM)
    return pl.pallas_call(
        functools.partial(kernel, sizes),
        out_shape=jax.ShapeDtypeStruct((query_count, block_rows), jnp.float32),
        in_specs=[anywhere] * 4,
        out_specs=pl.BlockSpec(memory_space=pltpu.VMEM),
        scratch_shapes=[
            pltpu.VMEM(queries.shape, queries.dtype),
            pltpu.VMEM((passage_count // 128, 128), passage_len.dtype),
            pltpu.VMEM((1, query_count), query_len.dtype),
            pltpu.VMEM(passages.shape, passages.dtype),
            pltpu.VMEM((2 * per_chunk * token_count, width), jnp.bfloat16),
            pltpu.VMEM((row_count, width), jnp.float32),
            pltpu.VMEM((width, row_count), jnp.bfloat16),
            pltpu.VMEM((passage_count, 128), jnp.float32),
            maxima,
            maxima,
            maxima,
            maxima,
            pltpu.VMEM((ny, chunks, per_chunk, query_count), jnp.float32),
            pltpu.VMEM((max(1, half_blocks - 1), block_rows, query_count), jnp.float32),
            pltpu.VMEM((block_rows, query_count), jnp.float32),
            pltpu.VMEM((nx * nz, 8, query_count), jnp.float32),
            dma((3,)),
            dma((2 * chunks,)),
            dma((2,)),
            dma((chunks, PARTS)),
            dma((chunks, PARTS)),
            dma((ny,)),
            dma((ny, half_blocks)),
            dma((max(1, half_blocks - 1),)),
            dma,
            dma((nx * nz,)),
            dma((nx * nz,)),
        ],
        compiler_params=pltpu.CompilerParams(
            collective_id=0, has_side_effects=True, vmem_limit_bytes=48 * 1024 * 1024
        ),
    )(
        queries,
        passage_len.reshape(passage_count // 128, 128),
        query_len.reshape(1, query_count),
        passages,
    )


def solution(mesh):
    sizes = tuple(mesh.shape[name] for name in ("gx", "gy", "gz"))
    return jax.shard_map(
        functools.partial(shards, sizes),
        mesh=mesh,
        in_specs=(P(None, "gy", None), P("gx", "gz", None), P("gx"), P()),
        out_specs=P(None, ("gx", "gz")),
        check_vma=False,
    )
```
